32 devices in a mesh: dp: 4 (over x, core), vocab: 8 (over z, y).
Axes of the slice: x: 2, y: 2, z: 4, core: 2. Of those that a mesh axis runs over, the one named last changes fastest.
Arguments:
- hidden: bfloat16 [256, 3584], P('dp'), may hold values from -160 to 160
- head_weight: bfloat16 [3584, 152064], P(None, ('dp', 'vocab')), may hold values from -0.3125 to 0.3125
- teacher_ids: int32 [256, 64], P('dp'), may hold values from 0 to 152063, as said below
- teacher_probs: float32 [256, 64], P('dp'), may hold values from 0 to 0.99, as said below
- token_weight: float32 [256], P('dp'), may hold values from 4 to 32
Outputs:
- divergence: float32 [256], P('dp')
- hidden_grad: float32 [256, 3584], P('dp', 'vocab')
The draws below stay inside these ranges and needn't reach their ends.
Inputs may be any that keep to these rules, and one draw needn't show every extreme that they name: `teacher_ids`: each row names 64 different vocabulary entries. `teacher_probs`: all positive; each row sums to between 0.5 and 0.99.
All inputs are finite; a program needn't handle non-finite values.
Results may differ from the reference program's by a relative error of at most 0.0029.
Values may be sent and summed in bfloat16 or wider, within the bound.
A program may use at most 128 MiB of HBM per device.

```python
import math
import jax
import jax.numpy as jnp
from jax import lax

D = 3584
V = 152064
TOP = 64
TOKENS = 256


def draw_hidden(key, part):
    base = jnp.clip(jax.random.normal(key, (TOKENS, D), jnp.float32), -4.0, 4.0)
    return base.astype(jnp.bfloat16)


def draw_teacher_ids(key, part):
    spread = jax.random.randint(key, (TOKENS, TOP), 0, V - TOP + 1, dtype=jnp.int32)
    ordered = jnp.sort(spread, axis=1) + jnp.arange(TOP, dtype=jnp.int32)[None, :]
    order_keys = jax.random.randint(jax.random.fold_in(key, 1), (TOKENS, TOP), 0, 1 << 20, dtype=jnp.int32) * TOP + jnp.arange(TOP, dtype=jnp.int32)[None, :]
    shuffle = jnp.argsort(order_keys, axis=1)
    return jnp.take_along_axis(ordered, shuffle, axis=1).astype(jnp.int32)


def draw_teacher_probs(key, part):
    raw = jnp.exp(jnp.clip(1.5 * jax.random.normal(key, (TOKENS, TOP), jnp.float32), -4.5, 4.5))
    totals = jax.random.uniform(jax.random.fold_in(key, 2), (TOKENS, 1), jnp.float32, 0.5, 0.99)
    return (totals * raw / jnp.sum(raw, axis=1, keepdims=True)).astype(jnp.float32)


def shard_levels(own_key, extent, cuts, low, top_value):
    gain, own = 1.0, jax.random.fold_in(own_key, 6)
    for position, parts in cuts:
        heights = jnp.exp(jax.random.uniform(jax.random.fold_in(own, position), (parts,), jnp.float32, low / len(cuts), top_value / len(cuts)))
        gain = gain * jnp.repeat(heights, extent[position] // parts).reshape([-1 if axis == position else 1 for axis in range(len(extent))])
    return gain


def centred(own_key, shape, scale, most, shards=(), kind=jnp.bfloat16):
    values = jax.random.normal(own_key, shape, jnp.float32) * scale
    if len(shards) > 0:
        values = shard_levels(own_key, shape, shards, -0.22, 0.18) * values
    return jnp.clip(values, min=-most, max=most).astype(kind)


def setup_inputs(seed: int = 0) -> dict:
    keys = jax.random.split(jax.random.key(seed), 6)
    hidden = draw_hidden(jax.random.fold_in(keys[5], 71), 0)
    head_weight = centred(keys[1], (D, V), (D // 9) ** -0.5, 0.3125, ((1, 32),))
    teacher_ids = draw_teacher_ids(jax.random.fold_in(keys[5], 71), 0)
    teacher_probs = draw_teacher_probs(jax.random.fold_in(keys[5], 71), 0)
    token_weight = jnp.clip(jnp.exp(math.log(32.0) - 2.0794415 * jax.random.uniform(keys[4], (TOKENS,), jnp.float32) ** shard_levels(keys[4], (TOKENS,), ((0, 4),), -0.2, 0.2)), 4.0, 32.0)
    return {"hidden": hidden, "head_weight": head_weight, "teacher_ids": teacher_ids, "teacher_probs": teacher_probs, "token_weight": token_weight}


def reference(hidden, head_weight, teacher_ids, teacher_probs, token_weight):
    block = math.gcd(TOKENS, 128)
    count = TOKENS // block

    def one_block(index):
        first = index * block
        rows_in = lax.dynamic_slice_in_dim(hidden, first, block, 0)
        chosen = lax.dynamic_slice_in_dim(teacher_ids, first, block, 0)
        probs = lax.dynamic_slice_in_dim(teacher_probs, first, block, 0)
        weights = lax.dynamic_slice_in_dim(token_weight, first, block, 0)
        logits = jnp.dot(rows_in, head_weight, preferred_element_type=jnp.float32)
        largest = jnp.max(logits, axis=1)
        expsum = jnp.sum(jnp.exp(logits - largest[:, None]), axis=1)
        log_norm = largest + jnp.log(expsum)
        picked = jnp.take_along_axis(logits, chosen, axis=1)
        mass = jnp.sum(probs, axis=1)
        divergence = jnp.sum(probs * (jnp.log(probs) - picked + log_norm[:, None]), axis=1)
        sparse = jnp.zeros(logits.shape, jnp.float32).at[jnp.arange(block)[:, None], chosen].add(probs)
        logit_grad = (mass[:, None] * jnp.exp(logits - log_norm[:, None]) - sparse).astype(jnp.bfloat16)
        backward = lax.dot_general(logit_grad, head_weight, (((1,), (1,)), ((), ())), preferred_element_type=jnp.float32)
        return divergence, weights[:, None] * backward

    divergence, hidden_grad = lax.map(one_block, jnp.arange(count, dtype=jnp.int32))
    return divergence.reshape(TOKENS), hidden_grad.reshape(TOKENS, D)
```

```python
import functools

import jax
import jax.numpy as jnp
from jax import lax
from jax.experimental import pallas as pl
from jax.experimental.pallas import tpu as pltpu
from jax.sharding import PartitionSpec as P

MESH = pl.DeviceIdType.MESH
NT = (((1,), (1,)), ((), ()))


def windows(feat):
    q = next(k for k in (1, 2, 4, 8, 16, 32, 64, 128) if k * feat % 128 == 0)
    first = [m * feat // 128 * 128 for m in range(q)]
    ww = max((m + 1) * feat - first[m] + 127 for m in range(q)) // 128 * 128
    return q, ww, [min(f, q * feat - ww) for f in first]


def kernel(
    ndp, nv, kc, hid, w, tp, tw, div_out, grad_out,
    wv, h_all, tp_all, sp, logits, lg, g, r1, s2, r2, stats, cols, cols2, back, own,
    w_sem, l_sem, hx_s, hx_r, hc_s, hc_r, tp_s, tp_r, st_s, st_r, g1_s, g1_r, g2_s, g2_r,
):
    d, mv = lax.axis_index("dp"), lax.axis_index("vocab")
    x, core = d // 2, d % 2
    nx, nd = ndp // 2, ndp * nv
    me = d * nv + mv
    rows, depth = hid.shape
    cols_n = w.shape[0]
    tok = rows * ndp
    nk = depth // kc
    nt = (cols_n + 127) // 128
    feat = depth // nv
    q, ww, starts = windows(feat)
    ng, group = nv // q, q * feat
    mg, mm = mv // q, lax.rem(mv, q)
    other = (2 * x + 1 - core, mv)

    def block(dp_index):
        return pl.ds(pl.multiple_of(dp_index * rows, rows), rows)

    def w_copy(c):
        part = pl.ds(pl.multiple_of(c * kc, kc), kc)
        return pltpu.make_async_copy(w.at[:, part], wv.at[:, part], w_sem.at[c])

    def l_copy():
        return pltpu.make_async_copy(hid, h_all.at[block(d), :], l_sem.at[0])

    def kpart(c):
        return pl.ds(pl.multiple_of(c * kc, kc), kc)

    def hx_copy(j, c):
        return pltpu.make_async_remote_copy(
            src_ref=hid.at[:, kpart(c)], dst_ref=h_all.at[block(d), kpart(c)],
            send_sem=hx_s.at[j - 1, c], recv_sem=hx_r.at[j - 1, c],
            device_id=(2 * lax.rem(x + j, nx) + core, mv), device_id_type=MESH)

    def hx_in(j, c):
        src = block(2 * lax.rem(x + nx - j, nx) + core)
        return pltpu.make_async_remote_copy(
            src_ref=h_all.at[src, kpart(c)], dst_ref=h_all.at[src, kpart(c)],
            send_sem=hx_s.at[j - 1, c], recv_sem=hx_r.at[j - 1, c],
            device_id=other, device_id_type=MESH)

    def hc_copy(j, c):
        if j == 0:
            src = hid.at[:, kpart(c)]
        else:
            src = h_all.at[block(2 * lax.rem(x + nx - j, nx) + core), kpart(c)]
        return pltpu.make_async_remote_copy(
            src_ref=src,
            dst_ref=h_all.at[block(2 * lax.rem(x + nx - j, nx) + core), kpart(c)],
            send_sem=hc_s.at[j, c], recv_sem=hc_r.at[j, c],
            device_id=other, device_id_type=MESH)

    def hc_in(j, c):
        dst = h_all.at[block(2 * lax.rem(x + nx - j, nx) + 1 - core), kpart(c)]
        return pltpu.make_async_remote_copy(
            src_ref=dst, dst_ref=dst, send_sem=hc_s.at[j, c], recv_sem=hc_r.at[j, c],
            device_id=other, device_id_type=MESH)

    def tp_copy(j, sender):
        return pltpu.make_async_remote_copy(
            src_ref=tp if sender is d else tp_all.at[block(sender), :],
            dst_ref=tp_all.at[block(sender), :],
            send_sem=tp_s.at[j - 1], recv_sem=tp_r.at[j - 1],
            device_id=(lax.rem(d + j, ndp), mv), device_id_type=MESH)

    def st_copy(j, sender):
        to = lax.rem(me + j, nd)
        return pltpu.make_async_remote_copy(
            src_ref=stats.at[sender], dst_ref=stats.at[sender],
            send_sem=st_s.at[j - 1], recv_sem=st_r.at[j - 1],
            device_id=(to // nv, lax.rem(to, nv)), device_id_type=MESH)

    def g1_copy(i, jx):
        theirs = block(2 * lax.rem(x + jx, nx) + 1 - core)
        return pltpu.make_async_remote_copy(
            src_ref=g.at[i, theirs, :], dst_ref=r1.at[i, jx],
            send_sem=g1_s.at[i, jx], recv_sem=g1_r.at[i, jx],
            device_id=other, device_id_type=MESH)

    def g2_copy(i, m, jx):
        return pltpu.make_async_remote_copy(
            src_ref=s2.at[i, m, jx], dst_ref=r2.at[i, mm, jx],
            send_sem=g2_s.at[i, m, jx], recv_sem=g2_r.at[i, mm, jx],
            device_id=(2 * lax.rem(x + jx, nx) + core, lax.rem(mg + 1 + i, ng) * q + m),
            device_id_type=MESH)

    def g2_in(i, m, jx):
        return pltpu.make_async_remote_copy(
            src_ref=r2.at[i, m, jx], dst_ref=r2.at[i, m, jx],
            send_sem=g2_s.at[i, m, jx], recv_sem=g2_r.at[i, m, jx],
            device_id=other, device_id_type=MESH)

    for c in range(nk):
        w_copy(c).start()
    l_copy().start()

    barrier = pltpu.get_barrier_semaphore()

    def greet(j, _):
        to = lax.rem(me + j, nd)
        pl.semaphore_signal(
            barrier, inc=1, device_id=(to // nv, lax.rem(to, nv)), device_id_type=MESH)
        return 0

    lax.fori_loop(1, nd, greet, 0)
    pl.semaphore_wait(barrier, nd - 1)

    for j in range(1, ndp):
        tp_copy(j, d).start()
    for c in range(nk):
        for j in range(1, nx):
            hx_copy(j, c).start()
        hc_copy(0, c).start()

    tp_all[block(d), :] = tp[...]
    for a in range(nt):
        logits[:, a * 128:(a + 1) * 128] = jnp.zeros((tok, 128), jnp.float32)
    if cols_n % 128:
        lane = lax.broadcasted_iota(jnp.int32, (tok, 128), 1)
        logits[:, (nt - 1) * 128:] = jnp.where(lane < cols_n % 128, 0.0, -1e30)
    for j in range(1, ndp):
        tp_copy(j, lax.rem(d + ndp - j, ndp)).wait_recv()

    offset = (me * cols_n).astype(jnp.float32)
    na = sp.shape[0] // tok
    iota_a = lax.broadcasted_iota(jnp.int32, (na, 128), 0)
    iota_b = lax.broadcasted_iota(jnp.int32, (128, 128), 0)
    lane8 = lax.broadcasted_iota(jnp.int32, (8, 128), 1)

    def build(step, _):
        t0 = pl.multiple_of(step * 8, 8)
        both = tp_all[pl.ds(t0, 8), :]
        turned = pltpu.roll(both, 64, 1)
        ids = jnp.where(lane8 < 64, both, turned)
        probs = jnp.where(lane8 < 64, turned, both)
        high = probs.astype(jnp.bfloat16).astype(jnp.float32)
        parts = jnp.where(lane8 < 64, high, probs - high)
        local = (ids - offset).astype(jnp.int32)
        inside = (local >= 0) & (local < cols_n)
        tile = jnp.where(inside, local >> 7, -1)
        low = local & 127
        for r in range(8):
            left = jnp.where(iota_a == tile[r:r + 1, :], parts[r:r + 1, :], 0.0)
            right = jnp.where(iota_b == low[r:r + 1, :], 1.0, 0.0)
            sp[pl.ds(t0 + r, na, stride=tok), :] = lax.dot_general(
                left.astype(jnp.bfloat16), right.astype(jnp.bfloat16), NT,
                preferred_element_type=jnp.float32)
        return 0

    lax.fori_loop(0, tok // 8, build, 0)

    def forward_in(c):
        for j in range(1, nx):
            hx_in(j, c).wait_recv()
            hc_copy(j, c).start()

    l_copy().wait()
    forward_in(0)
    wide = 512

    def first(c, _):
        @pl.when(c + 1 < nk)
        def _():
            forward_in(c + 1)

        for j in range(nx):
            hc_in(j, c).wait_recv()
        w_copy(c).wait()
        hc = h_all[:, kpart(c)]
        for n0 in range(0, cols_n, wide):
            n1 = min(n0 + wide, cols_n)
            logits[:, n0:n1] += lax.dot_general(
                hc, wv[n0:n1, kpart(c)], NT, preferred_element_type=jnp.float32)
        return 0

    lax.fori_loop(0, nk, first, 0)

    def peak(step, _):
        t0 = pl.multiple_of(step * 8, 8)
        ts = pl.ds(t0, 8)
        vals = [logits[ts, a * 128:(a + 1) * 128] for a in range(nt)]
        top = functools.reduce(jnp.maximum, vals)
        m = jnp.max(top, axis=1, keepdims=True)
        total = jnp.zeros((8, 128), jnp.float32)
        picked = jnp.zeros((8, 128), jnp.float32)
        for a in range(nt):
            picked += vals[a] * sp[pl.ds(a * tok + t0, 8), :]
            e = jnp.exp(vals[a] - m)
            logits[ts, a * 128:(a + 1) * 128] = e
            total += e
        s = jnp.sum(total, axis=1, keepdims=True)
        q = jnp.sum(picked, axis=1, keepdims=True)
        cols[ts, :] = jnp.where(lane8 == 0, m, jnp.where(lane8 == 1, s, q))
        return 0

    lax.fori_loop(0, tok // 8, peak, 0, unroll=2)

    turned_stats = cols[...].T
    for j in range(tok // 128):
        stats[me, 3 * j:3 * j + 3, :] = turned_stats[0:3, j * 128:(j + 1) * 128]
    for j in range(1, nd):
        st_copy(j, me).start()
    back[...] = jnp.zeros_like(back)
    for j in range(1, nd):
        st_copy(j, lax.rem(me + nd - j, nd)).wait_recv()
    for j in range(tok // 128):
        part = slice(j * 128, (j + 1) * 128)
        ms = stats[:, 3 * j, :]
        big = jnp.max(ms, axis=0, keepdims=True)
        z = jnp.sum(stats[:, 3 * j + 1, :] * jnp.exp(ms - big), axis=0, keepdims=True)
        back[0:1, part] = big + jnp.log(z)
        back[1:2, part] = jnp.sum(stats[:, 3 * j + 2, :], axis=0, keepdims=True)
    cols2[...] = back[...].T

    lane16 = lax.broadcasted_iota(jnp.int32, (16, 128), 1)

    def grad(step, _):
        t0 = pl.multiple_of(step * 16, 16)
        ts = pl.ds(t0, 16)
        mass = jnp.sum(jnp.where(lane16 >= 64, tp_all[ts, :], 0.0), axis=1, keepdims=True)
        scale = mass * jnp.exp(cols[ts, 0:1] - cols2[ts, 0:1])
        for a in range(nt):
            n1 = min(128, cols_n - a * 128)
            value = logits[ts, a * 128:(a + 1) * 128] * scale - sp[pl.ds(a * tok + t0, 16), :]
            lg[ts, a * 128:a * 128 + n1] = value[:, :n1].astype(jnp.bfloat16)
        return 0

    lax.fori_loop(0, tok // 16, grad, 0, unroll=2)

    def send_block(i, m, jx, both):
        s2[i, m, jx] = both[:, starts[m]:starts[m] + ww].astype(jnp.bfloat16)
        g2_copy(i, m, jx).start()

    def pass_on(i, last):
        for jx in range(nx):
            g1_copy(i, jx).wait_recv()
            mine = block(2 * lax.rem(x + jx, nx) + core)
            both = g[i, mine, :] + r1[i, jx]
            for m in range(q):
                if last and jx == 0:
                    @pl.when(m == mm)
                    def _():
                        own[...] = both[:, starts[m]:starts[m] + ww]

                    @pl.when(m != mm)
                    def _():
                        send_block(i, m, jx, both)
                else:
                    send_block(i, m, jx, both)

    def second(i, _):
        part = pl.ds(pl.multiple_of(lax.rem(mg + 1 + i, ng) * group, group), group)
        g[i] = jnp.dot(lg[...], wv[:, part], preferred_element_type=jnp.float32)
        for jx in range(nx):
            g1_copy(i, jx).start()

        @pl.when(i > 0)
        def _():
            pass_on(i - 1, False)

        return 0

    lax.fori_loop(0, ng, second, 0)
    pass_on(ng - 1, True)

    def not_own(i, m, jx):
        return (m != mm) if (i == ng - 1 and jx == 0) else (mm >= 0)

    mine = block(d)
    lane = lax.broadcasted_iota(jnp.int32, (rows, 128), 1)
    probs = jnp.where(lane >= 64, tp_all[mine, :], 1.0)
    entropy = jnp.sum(probs * jnp.log(probs), axis=1, keepdims=True)
    mass = jnp.sum(jnp.where(lane >= 64, probs, 0.0), axis=1, keepdims=True)
    div_out[...] = entropy - cols2[mine, 1:2] + mass * cols2[mine, 0:1]

    for i in range(ng):
        for jx in range(nx):
            for m in range(q):
                @pl.when(not_own(i, m, jx))
                def _():
                    g2_in(i, m, jx).wait_recv()
                    own[...] += r2[i, m, jx].astype(jnp.float32)
    for m in range(q):
        @pl.when(m == mm)
        def _():
            lo = m * feat - starts[m]
            grad_out[...] = own[:, lo:lo + feat] * tw[...]

    for c in range(nk):
        for j in range(1, nx):
            hx_copy(j, c).wait_send()
        for j in range(nx):
            hc_copy(j, c).wait_send()
    for j in range(1, ndp):
        tp_copy(j, d).wait_send()
    for j in range(1, nd):
        st_copy(j, me).wait_send()
    for i in range(ng):
        for jx in range(nx):
            g1_copy(i, jx).wait_send()
            for m in range(q):
                @pl.when(not_own(i, m, jx))
                def _():
                    g2_copy(i, m, jx).wait_send()


def body(ndp, nv, hidden, head_weight, teacher_ids, teacher_probs, token_weight):
    rows, depth = hidden.shape
    cols_n = head_weight.shape[1]
    tok, nx, nd, feat = rows * ndp, ndp // 2, ndp * nv, depth // nv
    q, ww, _ = windows(feat)
    ng, group = nv // q, q * feat
    kc = next(k for k in (512, 256, 128) if depth % k == 0)
    nk = depth // kc
    nt = (cols_n + 127) // 128
    na = (nt + 7) // 8 * 8
    srows = (3 * (tok // 128) + 7) // 8 * 8
    tp = jnp.concatenate([teacher_ids.astype(jnp.float32), teacher_probs], axis=1)
    f32, bf16, dma = jnp.float32, jnp.bfloat16, pltpu.SemaphoreType.DMA
    anyspace = pl.BlockSpec(memory_space=pl.ANY)
    vmem = pl.BlockSpec(memory_space=pltpu.VMEM)
    div, out = pl.pallas_call(
        functools.partial(kernel, ndp, nv, kc),
        out_shape=(
            jax.ShapeDtypeStruct((rows, 1), f32), jax.ShapeDtypeStruct((rows, feat), f32)),
        in_specs=[anyspace, anyspace, vmem, vmem],
        out_specs=(vmem, vmem),
        scratch_shapes=[
            pltpu.VMEM((cols_n, depth), bf16), pltpu.VMEM((tok, depth), bf16),
            pltpu.VMEM((tok, 128), f32), pltpu.VMEM((na * tok, 128), f32),
            pltpu.VMEM((tok, nt * 128), f32), pltpu.VMEM((tok, cols_n), bf16),
            pltpu.VMEM((ng, tok, group), f32), pltpu.VMEM((ng, nx, rows, group), f32),
            pltpu.VMEM((ng, q, nx, rows, ww), bf16), pltpu.VMEM((ng, q, nx, rows, ww), bf16),
            pltpu.VMEM((nd, srows, 128), f32), pltpu.VMEM((tok, 128), f32),
            pltpu.VMEM((tok, 128), f32), pltpu.VMEM((128, tok), f32),
            pltpu.VMEM((rows, ww), f32),
            dma((nk,)), dma((1,)), dma((nx - 1, nk)), dma((nx - 1, nk)),
            dma((nx, nk)), dma((nx, nk)), dma((ndp - 1,)), dma((ndp - 1,)),
            dma((nd - 1,)), dma((nd - 1,)), dma((ng, nx)), dma((ng, nx)),
            dma((ng, q, nx)), dma((ng, q, nx)),
        ],
        compiler_params=pltpu.CompilerParams(
            collective_id=0, has_side_effects=True, vmem_limit_bytes=67043328),
    )(hidden, head_weight.T, tp, token_weight[:, None])
    return div[:, 0], out


def solution(mesh):
    in_specs = (P("dp", None), P(None, ("dp", "vocab")), P("dp", None), P("dp", None), P("dp"))
    out_specs = (P("dp"), P("dp", "vocab"))
    return jax.shard_map(
        functools.partial(body, mesh.shape["dp"], mesh.shape["vocab"]),
        mesh=mesh, in_specs=in_specs, out_specs=out_specs, check_vma=False)
```

```python
import functools

import jax
import jax.numpy as jnp
from jax import lax
from jax.experimental import pallas as pl
from jax.experimental.pallas import tpu as pltpu
from jax.sharding import PartitionSpec as P

MESH = pl.DeviceIdType.MESH
NT = (((1,), (1,)), ((), ()))


def windows(feat):
    q = next(k for k in (1, 2, 4, 8, 16, 32, 64, 128) if k * feat % 128 == 0)
    first = [m * feat // 128 * 128 for m in range(q)]
    ww = max((m + 1) * feat - first[m] + 127 for m in range(q)) // 128 * 128
    return q, ww, [min(f, q * feat - ww) for f in first]


def kernel(
    ndp, nv, kc, hid, w, ids_in, probs_in, tw, div_out, grad_out,
    wv, h_all, tp_all, sp, logits, lg, g, r1, sx, rx, s2, r2, stats, cols, cols2, back, own,
    w_sem, l_sem, hx_s, hx_r, hc_s, hc_r, tp_s, tp_r, st_s, st_r, g1_s, g1_r, gx_s, gx_r, g2_s, g2_r,
):
    d, mv = lax.axis_index("dp"), lax.axis_index("vocab")
    x, core = d // 2, d % 2
    nx, nd = ndp // 2, ndp * nv
    me = d * nv + mv
    rows, depth = hid.shape
    cols_n = w.shape[0]
    tok = rows * ndp
    nk = depth // kc
    nt = (cols_n + 127) // 128
    feat = depth // nv
    q, ww, starts = windows(feat)
    ng, group = nv // q, q * feat
    mg, mm = mv // q, lax.rem(mv, q)
    other = (2 * x + 1 - core, mv)

    def block(dp_index):
        return pl.ds(pl.multiple_of(dp_index * rows, rows), rows)

    def w_copy(c):
        part = pl.ds(pl.multiple_of(c * kc, kc), kc)
        return pltpu.make_async_copy(w.at[:, part], wv.at[:, part], w_sem.at[c])

    def l_copy():
        return pltpu.make_async_copy(hid, h_all.at[block(d), :], l_sem.at[0])

    def kpart(c):
        return pl.ds(pl.multiple_of(c * kc, kc), kc)

    def hx_copy(j, c):
        return pltpu.make_async_remote_copy(
            src_ref=hid.at[:, kpart(c)], dst_ref=h_all.at[block(d), kpart(c)],
            send_sem=hx_s.at[j - 1, c], recv_sem=hx_r.at[j - 1, c],
            device_id=(2 * lax.rem(x + j, nx) + core, mv), device_id_type=MESH)

    def hx_in(j, c):
        src = block(2 * lax.rem(x + nx - j, nx) + core)
        return pltpu.make_async_remote_copy(
            src_ref=h_all.at[src, kpart(c)], dst_ref=h_all.at[src, kpart(c)],
            send_sem=hx_s.at[j - 1, c], recv_sem=hx_r.at[j - 1, c],
            device_id=other, device_id_type=MESH)

    def hc_copy(j, c):
        if j == 0:
            src = hid.at[:, kpart(c)]
        else:
            src = h_all.at[block(2 * lax.rem(x + nx - j, nx) + core), kpart(c)]
        return pltpu.make_async_remote_copy(
            src_ref=src,
            dst_ref=h_all.at[block(2 * lax.rem(x + nx - j, nx) + core), kpart(c)],
            send_sem=hc_s.at[j, c], recv_sem=hc_r.at[j, c],
            device_id=other, device_id_type=MESH)

    def hc_in(j, c):
        dst = h_all.at[block(2 * lax.rem(x + nx - j, nx) + 1 - core), kpart(c)]
        return pltpu.make_async_remote_copy(
            src_ref=dst, dst_ref=dst, send_sem=hc_s.at[j, c], recv_sem=hc_r.at[j, c],
            device_id=other, device_id_type=MESH)

    def tp_copy(j, sender):
        return pltpu.make_async_remote_copy(
            src_ref=tp_all.at[block(sender), :],
            dst_ref=tp_all.at[block(sender), :],
            send_sem=tp_s.at[j - 1], recv_sem=tp_r.at[j - 1],
            device_id=(lax.rem(d + j, ndp), mv), device_id_type=MESH)

    def st_copy(j, sender):
        to = lax.rem(me + j, nd)
        return pltpu.make_async_remote_copy(
            src_ref=stats.at[sender], dst_ref=stats.at[sender],
            send_sem=st_s.at[j - 1], recv_sem=st_r.at[j - 1],
            device_id=(to // nv, lax.rem(to, nv)), device_id_type=MESH)

    def g1_copy(i, jx):
        theirs = block(2 * lax.rem(x + jx, nx) + 1 - core)
        return pltpu.make_async_remote_copy(
            src_ref=g.at[i, theirs, :], dst_ref=r1.at[i, jx],
            send_sem=g1_s.at[i, jx], recv_sem=g1_r.at[i, jx],
            device_id=other, device_id_type=MESH)

    def gx_copy(i, jx):
        return pltpu.make_async_remote_copy(
            src_ref=sx.at[i, jx - 1], dst_ref=rx.at[i, jx - 1],
            send_sem=gx_s.at[i, jx - 1], recv_sem=gx_r.at[i, jx - 1],
            device_id=(2 * lax.rem(x + jx, nx) + core, mv), device_id_type=MESH)

    def g2_copy(i, m):
        return pltpu.make_async_remote_copy(
            src_ref=s2.at[i, m], dst_ref=r2.at[i, mm],
            send_sem=g2_s.at[i, m], recv_sem=g2_r.at[i, mm],
            device_id=(d, lax.rem(mg + 1 + i, ng) * q + m), device_id_type=MESH)

    def g2_in(i, m):
        return pltpu.make_async_remote_copy(
            src_ref=r2.at[i, m], dst_ref=r2.at[i, m],
            send_sem=g2_s.at[i, m], recv_sem=g2_r.at[i, m],
            device_id=other, device_id_type=MESH)

    for c in range(nk):
        w_copy(c).start()
    l_copy().start()

    top_n = ids_in.shape[1]
    tp_all[block(d), 0:top_n] = ids_in[...].astype(jnp.float32)
    tp_all[block(d), top_n:2 * top_n] = probs_in[...]

    barrier = pltpu.get_barrier_semaphore()

    def greet(j, _):
        to = lax.rem(me + j, nd)
        pl.semaphore_signal(
            barrier, inc=1, device_id=(to // nv, lax.rem(to, nv)), device_id_type=MESH)
        return 0

    lax.fori_loop(1, nd, greet, 0)
    pl.semaphore_wait(barrier, nd - 1)

    for j in range(1, ndp):
        tp_copy(j, d).start()
    for c in range(nk):
        for j in range(1, nx):
            hx_copy(j, c).start()
        hc_copy(0, c).start()

    for a in range(nt):
        logits[:, a * 128:(a + 1) * 128] = jnp.zeros((tok, 128), jnp.float32)
    if cols_n % 128:
        lane = lax.broadcasted_iota(jnp.int32, (tok, 128), 1)
        logits[:, (nt - 1) * 128:] = jnp.where(lane < cols_n % 128, 0.0, -1e30)
    for j in range(1, ndp):
        tp_copy(j, lax.rem(d + ndp - j, ndp)).wait_recv()

    offset = (me * cols_n).astype(jnp.float32)
    na = sp.shape[0] // tok
    iota_a = lax.broadcasted_iota(jnp.int32, (na, 128), 0)
    iota_b = lax.broadcasted_iota(jnp.int32, (128, 128), 0)
    lane8 = lax.broadcasted_iota(jnp.int32, (8, 128), 1)

    def build(step, _):
        t0 = pl.multiple_of(step * 8, 8)
        both = tp_all[pl.ds(t0, 8), :]
        turned = pltpu.roll(both, top_n, 1)
        ids = jnp.where(lane8 < top_n, both, turned)
        probs = jnp.where(lane8 < top_n, turned, both)
        high = probs.astype(jnp.bfloat16).astype(jnp.float32)
        parts = jnp.where(lane8 < top_n, high, probs - high)
        local = (ids - offset).astype(jnp.int32)
        inside = (local >= 0) & (local < cols_n)
        tile = jnp.where(inside, local >> 7, -1)
        low = local & 127
        for r in range(8):
            left = jnp.where(iota_a == tile[r:r + 1, :], parts[r:r + 1, :], 0.0)
            right = jnp.where(iota_b == low[r:r + 1, :], 1.0, 0.0)
            sp[pl.ds(t0 + r, na, stride=tok), :] = lax.dot_general(
                left.astype(jnp.bfloat16), right.astype(jnp.bfloat16), NT,
                preferred_element_type=jnp.float32)
        return 0

    lax.fori_loop(0, tok // 8, build, 0)

    def forward_in(c):
        for j in range(1, nx):
            hx_in(j, c).wait_recv()
            hc_copy(j, c).start()

    l_copy().wait()
    forward_in(0)
    wide = 512

    def first(c, _):
        @pl.when(c + 1 < nk)
        def _():
            forward_in(c + 1)

        for j in range(nx):
            hc_in(j, c).wait_recv()
        w_copy(c).wait()
        hc = h_all[:, kpart(c)]
        for n0 in range(0, cols_n, wide):
            n1 = min(n0 + wide, cols_n)
            logits[:, n0:n1] += lax.dot_general(
                hc, wv[n0:n1, kpart(c)], NT, preferred_element_type=jnp.float32)
        return 0

    lax.fori_loop(0, nk, first, 0)

    deep = 32
    lane_deep = lax.broadcasted_iota(jnp.int32, (deep, 128), 1)

    def peak(step, _):
        t0 = pl.multiple_of(step * deep, deep)
        ts = pl.ds(t0, deep)
        top = logits[ts, 0:128]
        for a in range(1, nt):
            top = jnp.maximum(top, logits[ts, a * 128:(a + 1) * 128])
        m = jnp.max(top, axis=1, keepdims=True)
        total = jnp.zeros((deep, 128), jnp.float32)
        picked = jnp.zeros((deep, 128), jnp.float32)
        for a in range(nt):
            value = logits[ts, a * 128:(a + 1) * 128]
            picked += value * sp[pl.ds(a * tok + t0, deep), :]
            e = jnp.exp(value - m)
            logits[ts, a * 128:(a + 1) * 128] = e
            total += e
        s = jnp.sum(total, axis=1, keepdims=True)
        q = jnp.sum(picked, axis=1, keepdims=True)
        cols[ts, :] = jnp.where(lane_deep == 0, m, jnp.where(lane_deep == 1, s, q))
        return 0

    lax.fori_loop(0, tok // deep, peak, 0)

    turned_stats = cols[...].T
    for j in range(tok // 128):
        stats[me, 3 * j:3 * j + 3, :] = turned_stats[0:3, j * 128:(j + 1) * 128]
    for j in range(1, nd):
        st_copy(j, me).start()
    back[...] = jnp.zeros_like(back)
    for j in range(1, nd):
        st_copy(j, lax.rem(me + nd - j, nd)).wait_recv()
    for j in range(tok // 128):
        part = slice(j * 128, (j + 1) * 128)
        ms = stats[:, 3 * j, :]
        big = jnp.max(ms, axis=0, keepdims=True)
        z = jnp.sum(stats[:, 3 * j + 1, :] * jnp.exp(ms - big), axis=0, keepdims=True)
        back[0:1, part] = big + jnp.log(z)
        back[1:2, part] = jnp.sum(stats[:, 3 * j + 2, :], axis=0, keepdims=True)
    cols2[...] = back[...].T

    lane16 = lax.broadcasted_iota(jnp.int32, (16, 128), 1)

    def grad(step, _):
        t0 = pl.multiple_of(step * 16, 16)
        ts = pl.ds(t0, 16)
        mass = jnp.sum(jnp.where(lane16 >= top_n, tp_all[ts, :], 0.0), axis=1, keepdims=True)
        scale = mass * jnp.exp(cols[ts, 0:1] - cols2[ts, 0:1])
        for a in range(nt):
            n1 = min(128, cols_n - a * 128)
            value = logits[ts, a * 128:(a + 1) * 128] * scale - sp[pl.ds(a * tok + t0, 16), :]
            lg[ts, a * 128:a * 128 + n1] = value[:, :n1].astype(jnp.bfloat16)
        return 0

    lax.fori_loop(0, tok // 16, grad, 0, unroll=2)

    def pair_sum(i, jx):
        g1_copy(i, jx).wait_recv()
        return g[i, block(2 * lax.rem(x + jx, nx) + core), :] + r1[i, jx]

    def to_x(i):
        for jx in range(1, nx):
            sx[i, jx - 1] = pair_sum(i, jx).astype(jnp.bfloat16)
            gx_copy(i, jx).start()

    def to_vocab(i, last):
        both = pair_sum(i, 0)
        for jx in range(1, nx):
            gx_copy(i, jx).wait_recv()
            both += rx[i, jx - 1].astype(jnp.float32)
        for m in range(q):
            def send_block():
                s2[i, m] = both[:, starts[m]:starts[m] + ww].astype(jnp.bfloat16)
                g2_copy(i, m).start()

            if last:
                @pl.when(m == mm)
                def _():
                    own[...] = both[:, starts[m]:starts[m] + ww]

                pl.when(m != mm)(send_block)
            else:
                send_block()

    def second(i, _):
        part = pl.ds(pl.multiple_of(lax.rem(mg + 1 + i, ng) * group, group), group)
        g[i] = jnp.dot(lg[...], wv[:, part], preferred_element_type=jnp.float32)
        for jx in range(nx):
            g1_copy(i, jx).start()

        @pl.when(i > 0)
        def _():
            to_x(i - 1)

        @pl.when(i > 1)
        def _():
            to_vocab(i - 2, False)

        return 0

    lax.fori_loop(0, ng, second, 0)
    to_x(ng - 1)
    if ng > 1:
        to_vocab(ng - 2, False)
    to_vocab(ng - 1, True)

    def not_own(i, m):
        return (m != mm) if i == ng - 1 else (mm >= 0)

    mine = block(d)
    lane = lax.broadcasted_iota(jnp.int32, (rows, 128), 1)
    probs = jnp.where(lane >= top_n, tp_all[mine, :], 1.0)
    entropy = jnp.sum(probs * jnp.log(probs), axis=1, keepdims=True)
    mass = jnp.sum(jnp.where(lane >= top_n, probs, 0.0), axis=1, keepdims=True)
    diagonal = lax.broadcasted_iota(jnp.int32, (rows, rows), 0) == (
        lax.broadcasted_iota(jnp.int32, (rows, rows), 1))
    column = entropy - cols2[mine, 1:2] + mass * cols2[mine, 0:1]
    div_out[...] = jnp.sum(jnp.where(diagonal, column, 0.0), axis=0, keepdims=True)
    weight = jnp.sum(jnp.where(diagonal, tw[...], 0.0), axis=1, keepdims=True)

    for i in range(ng):
        for m in range(q):
            @pl.when(not_own(i, m))
            def _():
                g2_in(i, m).wait_recv()
                own[...] += r2[i, m].astype(jnp.float32)
    for m in range(q):
        @pl.when(m == mm)
        def _():
            lo = m * feat - starts[m]
            grad_out[...] = own[:, lo:lo + feat] * weight

    for c in range(nk):
        for j in range(1, nx):
            hx_copy(j, c).wait_send()
        for j in range(nx):
            hc_copy(j, c).wait_send()
    for j in range(1, ndp):
        tp_copy(j, d).wait_send()
    for j in range(1, nd):
        st_copy(j, me).wait_send()
    for i in range(ng):
        for jx in range(nx):
            g1_copy(i, jx).wait_send()
        for jx in range(1, nx):
            gx_copy(i, jx).wait_send()
        for m in range(q):
            @pl.when(not_own(i, m))
            def _():
                g2_copy(i, m).wait_send()


def body(ndp, nv, hidden, head_weight, teacher_ids, teacher_probs, token_weight):
    rows, depth = hidden.shape
    cols_n = head_weight.shape[1]
    tok, nx, nd, feat = rows * ndp, ndp // 2, ndp * nv, depth // nv
    q, ww, _ = windows(feat)
    ng, group = nv // q, q * feat
    kc = next(k for k in (512, 256, 128) if depth % k == 0)
    nk = depth // kc
    nt = (cols_n + 127) // 128
    na = (nt + 7) // 8 * 8
    srows = (3 * (tok // 128) + 7) // 8 * 8
    f32, bf16, dma = jnp.float32, jnp.bfloat16, pltpu.SemaphoreType.DMA
    anyspace = pl.BlockSpec(memory_space=pl.ANY)
    vmem = pl.BlockSpec(memory_space=pltpu.VMEM)
    div, out = pl.pallas_call(
        functools.partial(kernel, ndp, nv, kc),
        out_shape=(
            jax.ShapeDtypeStruct((1, rows), f32), jax.ShapeDtypeStruct((rows, feat), f32)),
        in_specs=[anyspace, anyspace, vmem, vmem, vmem],
        out_specs=(vmem, vmem),
        scratch_shapes=[
            pltpu.VMEM((cols_n, depth), bf16), pltpu.VMEM((tok, depth), bf16),
            pltpu.VMEM((tok, 128), f32), pltpu.VMEM((na * tok, 128), f32),
            pltpu.VMEM((tok, nt * 128), f32), pltpu.VMEM((tok, cols_n), bf16),
            pltpu.VMEM((ng, tok, group), f32), pltpu.VMEM((ng, nx, rows, group), f32),
            pltpu.VMEM((ng, nx - 1, rows, group), bf16),
            pltpu.VMEM((ng, nx - 1, rows, group), bf16),
            pltpu.VMEM((ng, q, rows, ww), bf16), pltpu.VMEM((ng, q, rows, ww), bf16),
            pltpu.VMEM((nd, srows, 128), f32), pltpu.VMEM((tok, 128), f32),
            pltpu.VMEM((tok, 128), f32), pltpu.VMEM((128, tok), f32),
            pltpu.VMEM((rows, ww), f32),
            dma((nk,)), dma((1,)), dma((nx - 1, nk)), dma((nx - 1, nk)),
            dma((nx, nk)), dma((nx, nk)), dma((ndp - 1,)), dma((ndp - 1,)),
            dma((nd - 1,)), dma((nd - 1,)), dma((ng, nx)), dma((ng, nx)),
            dma((ng, nx - 1)), dma((ng, nx - 1)), dma((ng, q)), dma((ng, q)),
        ],
        compiler_params=pltpu.CompilerParams(
            collective_id=0, has_side_effects=True, vmem_limit_bytes=67043328),
    )(hidden, head_weight.T, teacher_ids, teacher_probs, token_weight[None, :])
    return div[0], out


def solution(mesh):
    in_specs = (P("dp", None), P(None, ("dp", "vocab")), P("dp", None), P("dp", None), P("dp"))
    out_specs = (P("dp"), P("dp", "vocab"))
    return jax.shard_map(
        functools.partial(body, mesh.shape["dp"], mesh.shape["vocab"]),
        mesh=mesh, in_specs=in_specs, out_specs=out_specs, check_vma=False)
```
